256 devices in a mesh: dp: 128 (over y, x, z), rep: 2 (over core).
Axes of the slice: x: 4, y: 4, z: 8, core: 2. Of those that a mesh axis runs over, the one named last changes fastest.
Arguments:
- tokens: bfloat16 [2, 1024, 4096], P('rep'), may hold values from -6 to 6
- cotangent: bfloat16 [2, 1024, 4096], P('rep'), may hold values from -6 to 6
- lengths: int32 [2, 2], P('rep'), may hold values from 1 to 512
- w_in: bfloat16 [4096, 2, 14336], P(None, None, 'dp'), may hold values from -0.09375 to 0.09375
- w_down: bfloat16 [14336, 4096], P('dp'), may hold values from -0.046875 to 0.046875
Outputs:
- d_tokens: float32 [2, 1024, 4096], P('rep', 'dp')
- weight_grads: float32 [4096, 3, 14336], P('rep', None, 'dp')
The draws below stay inside these ranges and needn't reach their ends.
All inputs are finite; a program needn't handle non-finite values.
Results may differ from the reference program's by a relative error of at most 0.0029.
Values sent between devices are 32-bit elements; how exact they have to be, the bound alone decides.
No kernel may reach another device: no remote copies, remote signals or barrier semaphores. Data moves between devices by JAX's collectives and lax.ppermute only.
A program may use at most 192 MiB of HBM per device.

```python
import jax
import jax.numpy as jnp

D = 4096
HID = 14336
ROWS = 1024
SEQS = 2
SLOTS = 512
N_REP = 2


def with_ends(entries, rng, low, high):
    place = [jax.random.randint(jax.random.fold_in(rng, axis), (), 0, length) for axis, length in enumerate(entries.shape)]
    longest = entries.shape.index(max(entries.shape))
    beside = place[:longest] + [(place[longest] + 1) % entries.shape[longest]] + place[longest + 1:]
    return entries.at[tuple(place)].set(low).at[tuple(beside)].set(high)


def levels(rng, extent, cuts, low, largest):
    def one(dim, shards_of):
        draws = jax.random.uniform(jax.random.fold_in(jax.random.fold_in(rng, 6), dim), (shards_of,), jnp.float32, low / len(cuts), largest / len(cuts))
        return jnp.repeat(jnp.exp(draws), extent[dim] // shards_of).reshape((-1,) + (1,) * (len(extent) - dim - 1))

    loudness = one(*cuts[0])
    for cut in cuts[1:]:
        loudness = loudness * one(*cut)
    return loudness


def centred(stream_key, dims, scale, bound, cuts=(), kind=jnp.bfloat16):
    values = scale * jax.random.normal(stream_key, dims, jnp.float32)
    if cuts:
        values = values * levels(stream_key, dims, cuts, -0.22, 0.18)
    return jnp.clip(values, -bound, bound).astype(kind)


def setup_inputs(seed: int = 0) -> dict:
    key_list = jax.random.split(jax.random.key(seed), 6)
    return {
        "tokens": centred(key_list[0], (N_REP, ROWS, D), 1.0, 6.0, ((0, 2),)),
        "cotangent": centred(key_list[1], (N_REP, ROWS, D), 1.0, 6.0, ((0, 2),)),
        "lengths": with_ends(jax.random.randint(key_list[2], (N_REP, SEQS), 1, SLOTS + 1), jax.random.fold_in(key_list[2], 1), 1, SLOTS).astype(jnp.int32),
        "w_in": centred(key_list[3], (D, 2, HID), D ** -0.5, 0.09375, ((2, 128),)),
        "w_down": centred(key_list[4], (HID, D), HID ** -0.5, 0.046875, ((0, 128),)),
    }


GRAD_SCALE = 0.03125


def reference(tokens, cotangent, lengths, w_in, w_down):
    hidden_units = w_down.shape[0]
    slots = ROWS // SEQS
    position = jnp.arange(ROWS)
    w_flat = w_in.reshape(D, 2 * hidden_units)
    zero_value = jnp.zeros((), jnp.bfloat16)
    total = jnp.zeros((D, 3, hidden_units), jnp.float32)
    results = []
    for replica in range(N_REP):
        limit = lengths[replica][position // slots]
        is_alive = (position % slots) < limit
        live_x = jnp.where(is_alive[:, None], tokens[replica], zero_value)
        live_dy = jnp.where(is_alive[:, None], cotangent[replica], zero_value)
        gate_up = jnp.dot(live_x, w_flat, preferred_element_type=jnp.float32)
        gate = gate_up[:, :hidden_units]
        upward = gate_up[:, hidden_units:]
        sigmoid_gate = jax.nn.sigmoid(gate)
        activated = gate * sigmoid_gate
        hidden = (activated * upward).astype(jnp.bfloat16)
        d_hidden = jnp.dot(live_dy, w_down.T, preferred_element_type=jnp.float32)
        d_gate = d_hidden * upward * sigmoid_gate * (1.0 + gate * (1.0 - sigmoid_gate))
        d_up = d_hidden * activated
        d_in = jnp.concatenate([d_gate, d_up], axis=1).astype(jnp.bfloat16)
        results.append(jnp.dot(d_in, w_flat.T, preferred_element_type=jnp.float32))
        grad_in = jnp.dot(live_x.T, d_in, preferred_element_type=jnp.float32)
        grad_down = jnp.dot(live_dy.T, hidden, preferred_element_type=jnp.float32)
        combined = jnp.concatenate([grad_in.reshape(D, 2, hidden_units), grad_down[:, None, :]], axis=1)
        total = total + combined * GRAD_SCALE
    return jnp.stack(results), total
```

```python
import jax
import jax.numpy as jnp
from jax import lax
from jax.sharding import Mesh
from jax.sharding import PartitionSpec as P

DP = ("dp_0", "dp_1", "dp_2")
ALL = DP + ("rep",)
GRAD_SCALE = 0.03125
LANES = 128
PAGE = 64
BUCKETS = (16, 19, 22, 32)


def ring_pairs(dims, axis_of_core, step):
    pairs = []
    ny, nx, nz, nr = dims
    for y in range(ny):
        for x in range(nx):
            for z in range(nz):
                for r in range(nr):
                    to = [y, x, z, r]
                    a = axis_of_core[r]
                    to[a] = (to[a] + step) % dims[a]
                    src = ((y * nx + x) * nz + z) * nr + r
                    dst = ((to[0] * nx + to[1]) * nz + to[2]) * nr + to[3]
                    pairs.append((src, dst))
    return pairs


def dot_t(a, b):
    return lax.dot_general(a, b, (((1,), (1,)), ((), ())), preferred_element_type=jnp.float32)


def dot_rows(a, b):
    return lax.dot_general(a, b, (((0,), (0,)), ((), ())), preferred_element_type=jnp.float32)


def rolled(value, start, dim):
    length = value.shape[dim]
    return lax.dynamic_slice_in_dim(jnp.concatenate([value, value], axis=dim), start, length, dim)


def row_sums(pages, d, w_sel, dims, beside):
    hop = lambda v, axes, step: lax.ppermute(v, ALL, ring_pairs(dims, axes, step))
    first, second = (1, 0), (0, 1)
    rows = pages * PAGE
    half = 2 * LANES
    depth = d.shape[0]
    w = lambda k, lo, hi: w_sel[:, k, lo:hi].reshape(depth, (hi - lo) * LANES)
    m1 = dot_rows(d, jnp.concatenate([w(2, 0, 2), w(1, 2, 4)], axis=1))
    m2 = dot_rows(d, jnp.concatenate([w(2, 2, 4), w(3, 0, 2)], axis=1))
    r1 = hop(m1, first, 1)
    r2 = hop(m2, first, -1)
    extra = beside()
    k1 = dot_rows(d, w(1, 0, 2))
    k2 = dot_rows(d, w(3, 2, 4))
    k0 = dot_rows(d, w(0, 0, 4))
    r1, r2, extra, k0, k1, k2 = lax.optimization_barrier((r1, r2, extra, k0, k1, k2))
    t1 = hop(k1 + r1[:, :half], first, 1)
    t2 = hop(k2 + r2[:, :half], first, -1)
    lo = k0[:, :half] + r2[:, half:] + t1
    hi = k0[:, half:] + r1[:, half:] + t2
    own, b1 = lo[:, :LANES], lo[:, LANES:]
    b2, b3 = hi[:, :LANES], hi[:, LANES:]
    mid = rows // 2
    r1 = hop(jnp.concatenate([b2[:mid], b1[mid:]]), second, 1)
    r2 = hop(jnp.concatenate([b2[mid:], b3[:mid]]), second, -1)
    t1 = hop(b1[:mid] + r1[:mid], second, 1)
    t2 = hop(b3[mid:] + r2[:mid], second, -1)
    top = own[:mid] + r2[mid:] + t1
    low = own[mid:] + r1[mid:] + t2
    mine = jnp.concatenate([top, low])
    nz = dims[2]
    tiles = mine.reshape(pages, nz, PAGE // nz, LANES).transpose(1, 0, 2, 3)
    tiles = lax.all_to_all(tiles, "dp_2", 0, 0, tiled=True)
    return jnp.sum(tiles, axis=0), extra


def one_hot(source, rows):
    return (source[:, None] == jnp.arange(rows)[None, :]).astype(jnp.bfloat16)


def per_device(tokens, cotangent, lengths, w_in, w_down, dims):
    ny, nx, nz, nr = dims
    x, dy = tokens[0], cotangent[0]
    rows, width = x.shape
    seqs = lengths.shape[1]
    slots = rows // seqs
    units = w_down.shape[0]
    rep = lax.axis_index("rep")
    iy, ix = lax.axis_index("dp_0"), lax.axis_index("dp_1")
    north = rep == 0
    per_seq = slots // PAGE

    theirs = lax.ppermute(lengths, "rep", [(0, 1), (1, 0)])
    w_t = w_in.transpose(1, 2, 0).reshape(2 * units, width)

    position = jnp.arange(rows)

    def mask(two):
        limit = jnp.where(position < slots, two[0, 0], two[0, 1])
        return (position % slots < limit)[None, :]

    is_alive = mask(lengths)
    gate_up = dot_t(w_t, x)
    gate, upward = gate_up[:units], gate_up[units:]
    sig = jax.nn.sigmoid(gate)
    activated = gate * sig
    hidden = jnp.where(is_alive, activated * upward, 0.0).astype(jnp.bfloat16)
    d_hidden = jnp.where(is_alive, dot_t(w_down, dy), 0.0)
    d_gate = d_hidden * upward * sig * (1.0 + gate * (1.0 - sig))
    d_up = d_hidden * activated
    mine = jnp.concatenate([d_gate, d_up], axis=0)
    d_in = mine.astype(jnp.bfloat16)
    other = lax.ppermute(mine, "rep", [(0, 1), (1, 0)])
    d_other = (other * mask(theirs).astype(jnp.float32)).astype(jnp.bfloat16)

    lens = [
        jnp.where(north, lengths[0, k], theirs[0, k]) for k in range(seqs)
    ] + [jnp.where(north, theirs[0, k], lengths[0, k]) for k in range(seqs)]
    live = [(length + PAGE - 1) // PAGE for length in lens]
    starts = [sum(live[:k], jnp.int32(0)) for k in range(nr * seqs)]
    total = starts[-1] + live[-1]

    my_first, my_second = jnp.where(north, ix, iy), jnp.where(north, iy, ix)
    w_mine = lax.dynamic_slice_in_dim(w_t, rep * (width // nr), width // nr, 1)
    w_sel = w_mine.reshape(2 * units, 4, 4, LANES)
    w_sel = rolled(rolled(w_sel, my_first, 1), my_second, 2)

    def branch(pages):
        def run(w_sel, x, dy, d_in, d_other, hidden):
            slot = jnp.arange(pages * PAGE)
            page = slot // PAGE
            source = [jnp.full_like(slot, -1), jnp.full_like(slot, -1)]
            for k in range(nr * seqs):
                here = (page >= starts[k]) & (page < starts[k] + live[k])
                at = slot - starts[k] * PAGE + (k % seqs) * slots
                source[k // seqs] = jnp.where(here, at, source[k // seqs])
            ours = jnp.where(north, source[0], source[1])
            peers = jnp.where(north, source[1], source[0])
            d = dot_t(d_in, one_hot(ours, rows)) + dot_t(d_other, one_hot(peers, rows))
            d = d.astype(jnp.bfloat16)

            def grads():
                g = jnp.concatenate(
                    [
                        jnp.dot(d_in, x, preferred_element_type=jnp.float32),
                        jnp.dot(hidden, dy, preferred_element_type=jnp.float32),
                    ]
                )
                low, high = g[:, : width // 2], g[:, width // 2 :]
                return jnp.where(north, high, low), jnp.where(north, low, high)

            done, (away, kept) = row_sums(pages, d, w_sel, dims, grads)
            got = lax.ppermute(away, "rep", [(0, 1), (1, 0)])
            shared = (kept + got) * GRAD_SCALE
            return jnp.pad(done, ((0, nr * rows // PAGE + per_seq - pages), (0, 0), (0, 0))), shared

        return run

    args = (w_sel, x, dy, d_in, d_other, hidden)
    if len(BUCKETS) == 1:
        done, shared = branch(BUCKETS[0])(*args)
    else:
        which = sum((total > b).astype(jnp.int32) for b in BUCKETS[:-1])
        done, shared = lax.switch(which, [branch(b) for b in BUCKETS], *args)

    outs = []
    for k in range(nr * seqs):
        part = lax.dynamic_slice_in_dim(done, starts[k], per_seq, 0)
        keep = jnp.arange(per_seq) < live[k]
        outs.append(jnp.where(keep[:, None, None], part, 0.0))
    sent = jnp.stack(outs).reshape(nr, seqs * per_seq, 8, LANES).transpose(1, 0, 2, 3)
    got = lax.all_to_all(sent.reshape(ny * nx * nr, 8, LANES), ("dp_0", "dp_1", "rep"), 0, 0, tiled=True)
    got = got.reshape(ny, nx, nr, 8, LANES)
    left = got[:, :, 0].transpose(2, 1, 0, 3).reshape(8, width // 2)
    right = got[:, :, 1].transpose(2, 0, 1, 3).reshape(8, width // 2)
    shard = jnp.concatenate([left, right], axis=1)
    weight_grads = shared.reshape(3, units, width // nr).transpose(2, 0, 1)
    return shard[None], weight_grads


def solution(mesh):
    dims = (4, 4, 8, mesh.shape["rep"])
    split = Mesh(mesh.devices.reshape(dims), ALL)
    in_specs = (
        P("rep", None, None),
        P("rep", None, None),
        P("rep", None),
        P(None, None, DP),
        P(DP, None),
    )
    out_specs = (P("rep", DP, None), P("rep", None, DP))
    return jax.shard_map(
        lambda *args: per_device(*args, dims),
        mesh=split, in_specs=in_specs, out_specs=out_specs, check_vma=False,
    )
```

```python
import jax
import jax.numpy as jnp
import numpy as np
from jax import lax
from jax.sharding import Mesh
from jax.sharding import PartitionSpec as P


DP = ("dp_0", "dp_1", "dp_2")
ALL = DP + ("rep",)
SWAP = [(0, 1), (1, 0)]
GRAD_SCALE = 0.03125
FIRST, SECOND = (1, 0), (0, 1)


def lines(dims, axis_of_core):
    index = np.arange(int(np.prod(dims))).reshape(dims)
    groups = []
    for core, axis in enumerate(axis_of_core):
        moved = np.moveaxis(index[..., core], axis, -1)
        groups += moved.reshape(-1, dims[axis]).tolist()
    return groups


def hop(value, dims, axis_of_core, step):
    pairs = []
    for line in lines(dims, axis_of_core):
        pairs += [(line[k], line[(k + step) % len(line)]) for k in range(len(line))]
    return lax.ppermute(value, ALL, sorted(pairs))


def exchange(value, dims, axis_of_core):
    groups = lines(dims, axis_of_core)
    return lax.all_to_all(value, ALL, 0, 0, tiled=True, axis_index_groups=groups)


def dot(a, b, over_a, over_b):
    return lax.dot_general(
        a, b, (((over_a,), (over_b,)), ((), ())), preferred_element_type=jnp.float32
    )


def per_device(tokens, cotangent, lengths, w_in, w_down, dims):
    ny, nx, nz, nr = dims
    x, dy = tokens[0], cotangent[0]
    rows, width = x.shape
    slots = rows // lengths.shape[1]
    units = w_down.shape[0]
    half = width // nr
    own_rows = rows // (ny * nx * nz)
    rep = lax.axis_index("rep")
    north = rep == 0
    me = jnp.where(north, lax.axis_index("dp_1"), lax.axis_index("dp_0"))
    one = jnp.minimum(lengths[0, 0], 1).astype(jnp.float32)

    w_t = w_in.transpose(1, 2, 0).reshape(2 * units, width)
    w_mine = lax.dynamic_slice_in_dim(w_t, rep * half, half, 1)
    w_gate, w_up = w_mine[:units].astype(jnp.float32), w_mine[units:].astype(jnp.float32)
    next_gate = hop(w_gate, dims, FIRST, -1)
    last_up = hop(w_up, dims, FIRST, 1)
    next_up = hop(w_up, dims, FIRST, -1)
    last_gate = hop(w_gate, dims, FIRST, 1)
    far_gate = hop(next_gate, dims, FIRST, -1)
    far_up = hop(last_up, dims, FIRST, 1)

    position = jnp.arange(rows)
    limit = jnp.where(position < slots, lengths[0, 0], slots + lengths[0, 1])
    is_alive = (position < limit)[None, :]
    gate_up = dot(w_t, x, 1, 1)
    gate, upward = gate_up[:units], gate_up[units:]
    sig = jax.nn.sigmoid(gate)
    activated = gate * sig
    hidden = jnp.where(is_alive, activated * upward, 0.0).astype(jnp.bfloat16)
    d_hidden = jnp.where(is_alive, dot(w_down, dy, 1, 1), 0.0)
    d_gate = d_hidden * upward * sig * (1.0 + gate * (1.0 - sig))
    d_up = d_hidden * activated
    d_in = jnp.concatenate([d_gate, d_up], axis=0).astype(jnp.bfloat16)

    each = rows // (ny * nx)
    order = (position // each % ny) * (nx * each) + (position // (ny * each)) * each + position % each
    turn = (position[:, None] == order[None, :]).astype(jnp.bfloat16)
    turned = dot(d_in, turn, 1, 0)
    plain = d_in.astype(jnp.float32)
    theirs = lax.ppermute(jnp.where(north, plain, turned), "rep", SWAP)
    ours = jnp.where(north, turned, plain)

    def spread(d):
        blocks = d.reshape(2 * units, 4, rows // 4).transpose(1, 0, 2)
        got = exchange(blocks, dims, FIRST)
        twice = jnp.concatenate([got, got])
        return (lax.dynamic_slice_in_dim(twice, me, 4, 0) * one).astype(jnp.bfloat16)

    d_theirs, d_ours = spread(theirs), spread(ours)

    g = jnp.concatenate([dot(d_in, x, 1, 0), dot(hidden, dy, 1, 0)])
    low, high = g[:, :half], g[:, half:]
    away, kept = jnp.where(north, high, low), jnp.where(north, low, high)
    back = lax.ppermute(away, "rep", SWAP)

    arrived = lambda *parts: [(p * one).astype(jnp.bfloat16) for p in parts]
    near = jnp.concatenate([w_mine] + arrived(next_gate, next_up, last_gate, last_up))
    far = jnp.concatenate(arrived(far_gate, far_up))

    def row_sums(d):
        close = jnp.concatenate([d[0], d[1], d[3]])
        partial = dot(close, near, 0, 0) + dot(d[2], far, 0, 0)
        got = exchange(partial.reshape(4, rows // 16, half), dims, SECOND)
        part = jnp.sum(got, axis=0).reshape(nz, own_rows, half)
        return jnp.sum(lax.all_to_all(part, "dp_2", 0, 0, tiled=True), axis=0)

    sum_theirs = row_sums(d_theirs)
    sum_ours = row_sums(d_ours)
    other_half = lax.ppermute(sum_theirs, "rep", SWAP)
    shard = jnp.concatenate(
        [jnp.where(north, sum_ours, other_half), jnp.where(north, other_half, sum_ours)], axis=1
    )
    shared = (kept + back) * GRAD_SCALE
    return shard[None], shared.reshape(3, units, half).transpose(2, 0, 1)


def solution(mesh):
    dims = (4, 4, 8, mesh.shape["rep"])
    split = Mesh(mesh.devices.reshape(dims), ALL)
    in_specs = (
        P("rep", None, None),
        P("rep", None, None),
        P("rep", None),
        P(None, None, DP),
        P(DP, None),
    )
    out_specs = (P("rep", DP, None), P("rep", None, DP))

    def body(*args):
        return per_device(*args, dims)

    return jax.shard_map(
        body, mesh=split, in_specs=in_specs, out_specs=out_specs, check_vma=False
    )
```

```python
import jax
import jax.numpy as jnp
import numpy as np
from jax import lax
from jax.sharding import Mesh
from jax.sharding import PartitionSpec as P


DP = ("dp_0", "dp_1", "dp_2")
ALL = DP + ("rep",)
SWAP = [(0, 1), (1, 0)]
GRAD_SCALE = 0.03125
FIRST, SECOND = (1, 0), (0, 1)


def lines(dims, axis_of_core):
    index = np.arange(int(np.prod(dims))).reshape(dims)
    groups = []
    for core, axis in enumerate(axis_of_core):
        moved = np.moveaxis(index[..., core], axis, -1)
        groups += moved.reshape(-1, dims[axis]).tolist()
    return groups


def hop(value, dims, axis_of_core, step):
    pairs = []
    for line in lines(dims, axis_of_core):
        pairs += [(line[k], line[(k + step) % len(line)]) for k in range(len(line))]
    return lax.ppermute(value, ALL, sorted(pairs))


def exchange(value, dims, axis_of_core):
    groups = lines(dims, axis_of_core)
    return lax.all_to_all(value, ALL, 0, 0, tiled=True, axis_index_groups=groups)


def dot(a, b, over_a, over_b):
    return lax.dot_general(
        a, b, (((over_a,), (over_b,)), ((), ())), preferred_element_type=jnp.float32
    )


def per_device(tokens, cotangent, lengths, w_in, w_down, dims):
    ny, nx, nz, nr = dims
    x, dy = tokens[0], cotangent[0]
    rows, width = x.shape
    slots = rows // lengths.shape[1]
    units = w_down.shape[0]
    half = width // nr
    own_rows = rows // (ny * nx * nz)
    rep = lax.axis_index("rep")
    north = rep == 0
    me = jnp.where(north, lax.axis_index("dp_1"), lax.axis_index("dp_0"))
    across = jnp.where(north, lax.axis_index("dp_0"), lax.axis_index("dp_1"))
    one = jnp.minimum(lengths[0, 0], 1).astype(jnp.float32)

    w_t = w_in.transpose(1, 2, 0).reshape(2 * units, width)
    w_mine = lax.dynamic_slice_in_dim(w_t, rep * half, half, 1)
    w_send = w_mine.astype(jnp.float32)
    w_next = hop(w_send, dims, FIRST, -1)
    w_last = hop(w_send, dims, FIRST, 1)
    far_gate = hop(w_next[:units], dims, FIRST, -1)
    far_up = hop(w_last[units:], dims, FIRST, 1)

    position = jnp.arange(rows)
    limit = jnp.where(position < slots, lengths[0, 0], slots + lengths[0, 1])
    is_alive = (position < limit)[None, :]
    gate_up = dot(w_t, x, 1, 1)
    gate, upward = gate_up[:units], gate_up[units:]
    sig = jax.nn.sigmoid(gate)
    activated = gate * sig
    hidden = jnp.where(is_alive, activated * upward, 0.0).astype(jnp.bfloat16)
    d_hidden = jnp.where(is_alive, dot(w_down, dy, 1, 1), 0.0)
    d_gate = d_hidden * upward * sig * (1.0 + gate * (1.0 - sig))
    d_up = d_hidden * activated
    d_in = jnp.concatenate([d_gate, d_up], axis=0).astype(jnp.bfloat16)

    each = rows // (ny * nx)
    order = (position // each % ny) * (nx * each) + (position // (ny * each)) * each + position % each
    turn = (position[:, None] == order[None, :]).astype(jnp.bfloat16)
    turned = dot(d_in, turn, 1, 0)
    plain = d_in.astype(jnp.float32)
    theirs = lax.ppermute(jnp.where(north, plain, turned), "rep", SWAP)
    ours = jnp.where(north, turned, plain)

    def spread(d):
        blocks = d.reshape(2 * units, 4, rows // 4).transpose(1, 0, 2)
        got = exchange(blocks, dims, FIRST)
        twice = jnp.concatenate([got, got])
        return (lax.dynamic_slice_in_dim(twice, me, 4, 0) * one).astype(jnp.bfloat16)

    d_theirs, d_ours = spread(theirs), spread(ours)

    g_in = dot(d_in, x, 1, 0)
    g_down = dot(hidden, dy, 1, 0)
    g = jnp.concatenate([g_in, g_down])
    low, high = g[:, :half], g[:, half:]
    away, kept = jnp.where(north, high, low), jnp.where(north, low, high)
    back = lax.ppermute(away, "rep", SWAP)

    arrived = lambda p: (p * one).astype(jnp.bfloat16)
    w_1, w_3 = arrived(w_next), arrived(w_last)
    w_2 = jnp.concatenate([arrived(far_gate), arrived(far_up)])
    cut = half // 2

    def row_sums(d):
        partial = dot(d[0], w_mine, 0, 0) + dot(d[1], w_1, 0, 0)
        partial = partial + dot(d[3], w_3, 0, 0) + dot(d[2], w_2, 0, 0)
        blocks = partial.reshape(4, rows // 16, half)
        blocks = jnp.concatenate([blocks, blocks])
        mine, b1, b2, b3 = (lax.dynamic_index_in_dim(blocks, across + k, 0, False) for k in range(4))
        r1 = hop(jnp.concatenate([b2[:, :cut], b1[:, cut:]], axis=1), dims, SECOND, 1)
        r2 = hop(jnp.concatenate([b3[:, :cut], b2[:, cut:]], axis=1), dims, SECOND, -1)
        t1 = hop(b1[:, :cut] + r1[:, :cut], dims, SECOND, 1)
        t2 = hop(b3[:, cut:] + r2[:, cut:], dims, SECOND, -1)
        left = mine[:, :cut] + r2[:, :cut] + t1
        right = mine[:, cut:] + r1[:, cut:] + t2
        part = jnp.concatenate([left, right], axis=1).reshape(nz, own_rows, half)
        got = lax.all_to_all(part, "dp_2", 0, 0, tiled=True)
        return jnp.sum(got, axis=0)

    sum_theirs = row_sums(d_theirs)
    sum_ours = row_sums(d_ours)
    other_half = lax.ppermute(sum_theirs, "rep", SWAP)
    shard = jnp.concatenate(
        [jnp.where(north, sum_ours, other_half), jnp.where(north, other_half, sum_ours)], axis=1
    )
    shared = (kept + back) * GRAD_SCALE
    return shard[None], shared.reshape(3, units, half).transpose(2, 0, 1)


def solution(mesh):
    dims = (4, 4, 8, mesh.shape["rep"])
    split = Mesh(mesh.devices.reshape(dims), ALL)
    in_specs = (
        P("rep", None, None),
        P("rep", None, None),
        P("rep", None),
        P(None, None, DP),
        P(DP, None),
    )
    out_specs = (P("rep", DP, None), P("rep", None, DP))

    def body(*args):
        return per_device(*args, dims)

    return jax.shard_map(
        body, mesh=split, in_specs=in_specs, out_specs=out_specs, check_vma=False
    )
```

```python
import jax
import jax.numpy as jnp
import numpy as np
from jax import lax
from jax.sharding import Mesh
from jax.sharding import PartitionSpec as P


DP = ("dp_0", "dp_1", "dp_2")
ALL = DP + ("rep",)
SWAP = [(0, 1), (1, 0)]
GRAD_SCALE = 0.03125
FIRST, SECOND = (1, 0), (0, 1)


def lines(dims, axis_of_core):
    index = np.arange(int(np.prod(dims))).reshape(dims)
    groups = []
    for core, axis in enumerate(axis_of_core):
        moved = np.moveaxis(index[..., core], axis, -1)
        groups += moved.reshape(-1, dims[axis]).tolist()
    return groups


def hop(value, dims, axis_of_core, step):
    pairs = []
    for line in lines(dims, axis_of_core):
        pairs += [(line[k], line[(k + step) % len(line)]) for k in range(len(line))]
    return lax.ppermute(value, ALL, sorted(pairs))


def exchange(value, dims, axis_of_core):
    groups = lines(dims, axis_of_core)
    return lax.all_to_all(value, ALL, 0, 0, tiled=True, axis_index_groups=groups)


def dot(a, b, over_a, over_b):
    return lax.dot_general(
        a, b, (((over_a,), (over_b,)), ((), ())), preferred_element_type=jnp.float32
    )


def per_device(tokens, cotangent, lengths, w_in, w_down, dims):
    ny, nx, nz, nr = dims
    x, dy = tokens[0], cotangent[0]
    rows, width = x.shape
    slots = rows // lengths.shape[1]
    units = w_down.shape[0]
    half = width // nr
    own_rows = rows // (ny * nx * nz)
    rep = lax.axis_index("rep")
    north = rep == 0
    me = jnp.where(north, lax.axis_index("dp_1"), lax.axis_index("dp_0"))
    across = jnp.where(north, lax.axis_index("dp_0"), lax.axis_index("dp_1"))
    one = jnp.minimum(lengths[0, 0], 1).astype(jnp.float32)

    w_t = w_in.transpose(1, 2, 0).reshape(2 * units, width)
    w_mine = jnp.where(north, w_t[:, :half], w_t[:, half:])
    w_gate, w_up = w_mine[:units].astype(jnp.float32), w_mine[units:].astype(jnp.float32)
    next_gate = hop(w_gate, dims, FIRST, -1)
    last_up = hop(w_up, dims, FIRST, 1)
    next_up = hop(w_up, dims, FIRST, -1)
    last_gate = hop(w_gate, dims, FIRST, 1)
    far_gate = hop(next_gate, dims, FIRST, -1)
    far_up = hop(last_up, dims, FIRST, 1)

    position = jnp.arange(rows)
    limit = jnp.where(position < slots, lengths[0, 0], slots + lengths[0, 1])
    is_alive = (position < limit)[None, :]
    gate_up = dot(w_t, x, 1, 1)
    gate, upward = gate_up[:units], gate_up[units:]
    sig = jax.nn.sigmoid(gate)
    activated = gate * sig
    hidden = jnp.where(is_alive, activated * upward, 0.0).astype(jnp.bfloat16)
    d_hidden = jnp.where(is_alive, dot(w_down, dy, 1, 1), 0.0)
    d_gate = d_hidden * upward * sig * (1.0 + gate * (1.0 - sig))
    d_up = d_hidden * activated
    d_in = jnp.concatenate([d_gate, d_up], axis=0).astype(jnp.bfloat16)

    each = rows // (ny * nx)
    order = (position // each % ny) * (nx * each) + (position // (ny * each)) * each + position % each
    turn = (position[:, None] == order[None, :]).astype(jnp.bfloat16)
    turned = dot(d_in, turn, 1, 0)
    plain = d_in.astype(jnp.float32)
    theirs = lax.ppermute(jnp.where(north, plain, turned), "rep", SWAP)
    ours = jnp.where(north, turned, plain)

    cols = rows // 4
    blocks = [jnp.concatenate([d[:, k * cols : (k + 1) * cols] for d in (ours, theirs)]) for k in range(4)]
    got = exchange(jnp.stack(blocks), dims, FIRST)
    got = lax.dynamic_slice_in_dim(jnp.concatenate([got, got]), me, 4, 0)
    d_all = (got * one).astype(jnp.bfloat16)

    g_in = dot(d_in, x, 1, 0)
    g_down = dot(hidden, dy, 1, 0)
    g = jnp.concatenate([g_in, g_down])
    low, high = g[:, :half], g[:, half:]
    away, kept = jnp.where(north, high, low), jnp.where(north, low, high)
    back = lax.ppermute(away, "rep", SWAP)

    arrived = lambda p: (p * one).astype(jnp.bfloat16)
    w_1 = jnp.concatenate([arrived(next_gate), arrived(next_up)])
    w_2 = jnp.concatenate([arrived(far_gate), arrived(far_up)])
    w_3 = jnp.concatenate([arrived(last_gate), arrived(last_up)])
    cut = half // 2

    def row_sums(d):
        partial = dot(d[0], w_mine, 0, 0) + dot(d[1], w_1, 0, 0)
        partial = partial + dot(d[3], w_3, 0, 0) + dot(d[2], w_2, 0, 0)
        blocks = partial.reshape(4, rows // 16, half)
        blocks = jnp.concatenate([blocks, blocks])
        mine, b1, b2, b3 = (lax.dynamic_index_in_dim(blocks, across + k, 0, False) for k in range(4))
        r1 = hop(jnp.concatenate([b2[:, :cut], b1[:, cut:]], axis=1), dims, SECOND, 1)
        r2 = hop(jnp.concatenate([b3[:, :cut], b2[:, cut:]], axis=1), dims, SECOND, -1)
        up, down = b1[:, :cut] + r1[:, :cut], b3[:, cut:] + r2[:, cut:]
        t1 = hop(up, dims, SECOND, 1)
        t2 = hop(down, dims, SECOND, -1)
        left = mine[:, :cut] + r2[:, :cut] + t1
        right = mine[:, cut:] + r1[:, cut:] + t2
        part = jnp.concatenate([left, right], axis=1).reshape(nz, own_rows, half)
        got = lax.all_to_all(part, "dp_2", 0, 0, tiled=True)
        return jnp.sum(got, axis=0)

    sum_theirs = row_sums(d_all[:, 2 * units :])
    sum_ours = row_sums(d_all[:, : 2 * units])
    other_half = lax.ppermute(sum_theirs, "rep", SWAP)
    shard = jnp.concatenate(
        [jnp.where(north, sum_ours, other_half), jnp.where(north, other_half, sum_ours)], axis=1
    )
    shared = (kept + back) * GRAD_SCALE
    return shard[None], shared.reshape(3, units, half).transpose(2, 0, 1)


def solution(mesh):
    dims = (4, 4, 8, mesh.shape["rep"])
    split = Mesh(mesh.devices.reshape(dims), ALL)
    in_specs = (
        P("rep", None, None),
        P("rep", None, None),
        P("rep", None),
        P(None, None, DP),
        P(DP, None),
    )
    out_specs = (P("rep", DP, None), P("rep", None, DP))

    def body(*args):
        return per_device(*args, dims)

    return jax.shard_map(
        body, mesh=split, in_specs=in_specs, out_specs=out_specs, check_vma=False
    )
```

```python
import jax
import jax.numpy as jnp
import numpy as np
from jax import lax
from jax.sharding import Mesh
from jax.sharding import PartitionSpec as P


DP = ("dp_0", "dp_1", "dp_2")
ALL = DP + ("rep",)
SWAP = [(0, 1), (1, 0)]
GRAD_SCALE = 0.03125
FIRST, SECOND = (1, 0), (0, 1)


def lines(dims, axis_of_core):
    index = np.arange(int(np.prod(dims))).reshape(dims)
    groups = []
    for core, axis in enumerate(axis_of_core):
        moved = np.moveaxis(index[..., core], axis, -1)
        groups += moved.reshape(-1, dims[axis]).tolist()
    return groups


def hop(value, dims, axis_of_core, step):
    pairs = []
    for line in lines(dims, axis_of_core):
        pairs += [(line[k], line[(k + step) % len(line)]) for k in range(len(line))]
    return lax.ppermute(value, ALL, sorted(pairs))


def exchange(value, dims, axis_of_core):
    groups = lines(dims, axis_of_core)
    return lax.all_to_all(value, ALL, 0, 0, tiled=True, axis_index_groups=groups)


def dot(a, b, over_a, over_b):
    return lax.dot_general(
        a, b, (((over_a,), (over_b,)), ((), ())), preferred_element_type=jnp.float32
    )


def per_device(tokens, cotangent, lengths, w_in, w_down, dims):
    ny, nx, nz, nr = dims
    x, dy = tokens[0], cotangent[0]
    rows, width = x.shape
    slots = rows // lengths.shape[1]
    units = w_down.shape[0]
    half = width // nr
    own_rows = rows // (ny * nx * nz)
    rep = lax.axis_index("rep")
    north = rep == 0
    me = jnp.where(north, lax.axis_index("dp_1"), lax.axis_index("dp_0"))
    across = jnp.where(north, lax.axis_index("dp_0"), lax.axis_index("dp_1"))
    one = jnp.minimum(lengths[0, 0], 1).astype(jnp.float32)

    w_t = w_in.transpose(1, 2, 0).reshape(2 * units, width)
    w_mine = lax.dynamic_slice_in_dim(w_t, rep * half, half, 1)
    mine_of = lambda part: jnp.where(north, part[:, :half], part[:, half:]).astype(jnp.float32)
    w_gate, w_up = mine_of(w_t[:units]), mine_of(w_t[units:])
    next_gate = hop(w_gate, dims, FIRST, -1)
    last_up = hop(w_up, dims, FIRST, 1)
    next_up = hop(w_up, dims, FIRST, -1)
    last_gate = hop(w_gate, dims, FIRST, 1)
    far_gate = hop(next_gate, dims, FIRST, -1)
    far_up = hop(last_up, dims, FIRST, 1)

    position = jnp.arange(rows)
    limit = jnp.where(position < slots, lengths[0, 0], slots + lengths[0, 1])
    is_alive = (position < limit)[None, :]
    gate_up = dot(w_t, x, 1, 1)
    gate, upward = gate_up[:units], gate_up[units:]
    sig = jax.nn.sigmoid(gate)
    activated = gate * sig
    hidden = jnp.where(is_alive, activated * upward, 0.0).astype(jnp.bfloat16)
    d_hidden = dot(w_down, dy, 1, 1)
    d_hidden = jnp.where(is_alive, d_hidden, 0.0)
    d_gate = d_hidden * upward * sig * (1.0 + gate * (1.0 - sig))
    d_up = d_hidden * activated
    d_in = jnp.concatenate([d_gate, d_up], axis=0).astype(jnp.bfloat16)

    each = rows // (ny * nx)
    order = (position // each % ny) * (nx * each) + (position // (ny * each)) * each + position % each
    turn = (position[:, None] == order[None, :]).astype(jnp.bfloat16)
    turned = dot(d_in, turn, 1, 0)
    plain = d_in.astype(jnp.float32)
    away, ours = jnp.where(north, plain, turned), jnp.where(north, turned, plain)
    theirs = lax.ppermute(away, "rep", SWAP)

    cols = rows // 4
    blocks = [jnp.concatenate([d[:, k * cols : (k + 1) * cols] for d in (ours, theirs)]) for k in range(4)]
    got = exchange(jnp.stack(blocks), dims, FIRST)
    picked = [lax.dynamic_index_in_dim(got, (me + k) & 3, 0, False) for k in range(4)]
    d_all = [(d * one).astype(jnp.bfloat16) for d in picked]

    g_in = dot(d_in, x, 1, 0)
    g_down = dot(hidden, dy, 1, 0)
    g = jnp.concatenate([g_in, g_down])
    low, high = g[:, :half], g[:, half:]
    away, kept = jnp.where(north, high, low), jnp.where(north, low, high)
    back = lax.ppermute(away, "rep", SWAP)

    arrived = lambda p: (p * one).astype(jnp.bfloat16)
    w_1 = jnp.concatenate([arrived(next_gate), arrived(next_up)])
    w_2 = jnp.concatenate([arrived(far_gate), arrived(far_up)])
    w_3 = jnp.concatenate([arrived(last_gate), arrived(last_up)])
    cut = half // 2

    def product(r):
        at = ((r + rep) & 1) * 2 * units
        d = [lax.dynamic_slice_in_dim(value, at, 2 * units, 0) for value in d_all]
        partial = dot(d[0], w_mine, 0, 0) + dot(d[1], w_1, 0, 0)
        partial = partial + dot(d[3], w_3, 0, 0) + dot(d[2], w_2, 0, 0)
        return partial.reshape(4, rows // 16, half)

    products = [product(r) for r in range(nr)]
    mine, b1, b2, b3 = (
        jnp.concatenate([lax.dynamic_index_in_dim(p, (across + k) & 3, 0, False) for p in products])
        for k in range(4)
    )
    r1 = hop(jnp.concatenate([b2[:, :cut], b1[:, cut:]], axis=1), dims, SECOND, 1)
    r2 = hop(jnp.concatenate([b3[:, :cut], b2[:, cut:]], axis=1), dims, SECOND, -1)
    up_2, down_2 = lax.optimization_barrier((b1[:, :cut] + r1[:, :cut], b3[:, cut:] + r2[:, cut:]))
    t1 = hop(up_2, dims, SECOND, 1)
    t2 = hop(down_2, dims, SECOND, -1)
    left = mine[:, :cut] + r2[:, :cut] + t1
    right = mine[:, cut:] + r1[:, cut:] + t2
    part = jnp.concatenate([left, right], axis=1).reshape(nr, nz, own_rows, half)
    part = part.transpose(1, 0, 2, 3).reshape(nz * nr, own_rows, half)
    got = lax.all_to_all(part, ("dp_2", "rep"), 0, 0, tiled=True)
    shard = jnp.sum(got.reshape(nz, nr, own_rows, half), axis=0)
    shard = shard.transpose(1, 0, 2).reshape(own_rows, width)
    shared = (kept + back) * GRAD_SCALE
    return shard[None], shared.reshape(3, units, half).transpose(2, 0, 1)


def solution(mesh):
    dims = (4, 4, 8, mesh.shape["rep"])
    split = Mesh(mesh.devices.reshape(dims), ALL)
    in_specs = (
        P("rep", None, None),
        P("rep", None, None),
        P("rep", None),
        P(None, None, DP),
        P(DP, None),
    )
    out_specs = (P("rep", DP, None), P("rep", None, DP))

    def body(*args):
        return per_device(*args, dims)

    return jax.shard_map(
        body, mesh=split, in_specs=in_specs, out_specs=out_specs, check_vma=False
    )
```

```python
import jax
import jax.numpy as jnp
import numpy as np
from jax import lax
from jax.sharding import Mesh
from jax.sharding import PartitionSpec as P


DP = ("dp_0", "dp_1", "dp_2")
ALL = DP + ("rep",)
SWAP = [(0, 1), (1, 0)]
GRAD_SCALE = 0.03125
CHUNKS = 2
FIRST, SECOND = (1, 0), (0, 1)


def lines(dims, axis_of_core):
    index = np.arange(int(np.prod(dims))).reshape(dims)
    groups = []
    for core, axis in enumerate(axis_of_core):
        moved = np.moveaxis(index[..., core], axis, -1)
        groups += moved.reshape(-1, dims[axis]).tolist()
    return groups


def hop(value, dims, axis_of_core, step):
    pairs = []
    for line in lines(dims, axis_of_core):
        pairs += [(line[k], line[(k + step) % len(line)]) for k in range(len(line))]
    return lax.ppermute(value, ALL, sorted(pairs))


def exchange(value, dims, axis_of_core):
    groups = lines(dims, axis_of_core)
    return lax.all_to_all(value, ALL, 0, 0, tiled=True, axis_index_groups=groups)


def dot(a, b, over_a, over_b):
    return lax.dot_general(
        a, b, (((over_a,), (over_b,)), ((), ())), preferred_element_type=jnp.float32
    )


def per_device(tokens, cotangent, lengths, w_in, w_down, dims):
    ny, nx, nz, nr = dims
    x, dy = tokens[0], cotangent[0]
    rows, width = x.shape
    slots = rows // lengths.shape[1]
    units = w_down.shape[0]
    half = width // nr
    own_rows = rows // (ny * nx * nz)
    rep = lax.axis_index("rep")
    north = rep == 0
    me = jnp.where(north, lax.axis_index("dp_1"), lax.axis_index("dp_0"))
    across = jnp.where(north, lax.axis_index("dp_0"), lax.axis_index("dp_1"))
    one = jnp.minimum(lengths[0, 0], 1).astype(jnp.float32)

    w_t = w_in.transpose(1, 2, 0).reshape(2 * units, width)
    cut = half // CHUNKS
    w_mine, near, far = [], [], []
    for c in range(CHUNKS):
        w_mine.append(lax.dynamic_slice_in_dim(w_t, rep * half + c * cut, cut, 1))
        sent = w_mine[c].astype(jnp.float32)
        w_next = hop(sent, dims, FIRST, -1)
        w_last = hop(sent, dims, FIRST, 1)
        far_gate = hop(w_next[:units], dims, FIRST, -1)
        far_up = hop(w_last[units:], dims, FIRST, 1)
        near.append((w_next, w_last))
        far.append((far_gate, far_up))

    position = jnp.arange(rows)
    limit = jnp.where(position < slots, lengths[0, 0], slots + lengths[0, 1])
    is_alive = (position < limit)[None, :]
    gate_up = dot(w_t, x, 1, 1)
    gate, upward = gate_up[:units], gate_up[units:]
    sig = jax.nn.sigmoid(gate)
    activated = gate * sig
    hidden = jnp.where(is_alive, activated * upward, 0.0).astype(jnp.bfloat16)
    d_hidden = dot(w_down, dy, 1, 1)
    d_hidden = jnp.where(is_alive, d_hidden, 0.0)
    d_gate = d_hidden * upward * sig * (1.0 + gate * (1.0 - sig))
    d_up = d_hidden * activated
    d_in = jnp.concatenate([d_gate, d_up], axis=0).astype(jnp.bfloat16)

    each = rows // (ny * nx)
    order = (position // each % ny) * (nx * each) + (position // (ny * each)) * each + position % each
    turn = (position[:, None] == order[None, :]).astype(jnp.bfloat16)
    turned = dot(d_in, turn, 1, 0)
    plain = d_in.astype(jnp.float32)
    away, ours = jnp.where(north, plain, turned), jnp.where(north, turned, plain)
    theirs = lax.ppermute(away, "rep", SWAP)

    cols = rows // 4
    blocks = [jnp.concatenate([d[:, k * cols : (k + 1) * cols] for d in (ours, theirs)]) for k in range(4)]
    got = exchange(jnp.stack(blocks), dims, FIRST)
    picked = [lax.dynamic_index_in_dim(got, (me + k) & 3, 0, False) for k in range(4)]
    d_all = [(d * one).astype(jnp.bfloat16) for d in picked]

    g_in = dot(d_in, x, 1, 0)
    g_down = dot(hidden, dy, 1, 0)
    g = jnp.concatenate([g_in, g_down])
    low, high = g[:, :half], g[:, half:]
    away, kept = jnp.where(north, high, low), jnp.where(north, low, high)
    back = lax.ppermute(away, "rep", SWAP)

    arrived = lambda p: (p * one).astype(jnp.bfloat16)
    edge = cut // 2
    halves = []
    for c in range(CHUNKS):
        w_1, w_3 = arrived(near[c][0]), arrived(near[c][1])
        w_2 = jnp.concatenate([arrived(far[c][0]), arrived(far[c][1])])

        def product(r):
            at = ((r + rep) & 1) * 2 * units
            d = [lax.dynamic_slice_in_dim(value, at, 2 * units, 0) for value in d_all]
            partial = dot(d[0], w_mine[c], 0, 0) + dot(d[1], w_1, 0, 0)
            partial = partial + dot(d[3], w_3, 0, 0) + dot(d[2], w_2, 0, 0)
            return partial.reshape(4, rows // 16, cut)

        products = [product(r) for r in range(nr)]
        mine, b1, b2, b3 = (
            jnp.concatenate([lax.dynamic_index_in_dim(p, (across + k) & 3, 0, False) for p in products])
            for k in range(4)
        )
        r1 = hop(jnp.concatenate([b2[:, :edge], b1[:, edge:]], axis=1), dims, SECOND, 1)
        r2 = hop(jnp.concatenate([b3[:, :edge], b2[:, edge:]], axis=1), dims, SECOND, -1)
        up, down = lax.optimization_barrier((b1[:, :edge] + r1[:, :edge], b3[:, edge:] + r2[:, edge:]))
        t1 = hop(up, dims, SECOND, 1)
        t2 = hop(down, dims, SECOND, -1)
        left = mine[:, :edge] + r2[:, :edge] + t1
        right = mine[:, edge:] + r1[:, edge:] + t2
        part = jnp.concatenate([left, right], axis=1).reshape(nr, nz, own_rows, cut)
        part = part.transpose(1, 0, 2, 3).reshape(nz * nr, own_rows, cut)
        got = lax.all_to_all(part, ("dp_2", "rep"), 0, 0, tiled=True)
        halves.append(jnp.sum(got.reshape(nz, nr, own_rows, cut), axis=0))
    shard = jnp.concatenate([h[r] for r in range(nr) for h in halves], axis=1)
    shared = (kept + back) * GRAD_SCALE
    return shard[None], shared.reshape(3, units, half).transpose(2, 0, 1)


def solution(mesh):
    dims = (4, 4, 8, mesh.shape["rep"])
    split = Mesh(mesh.devices.reshape(dims), ALL)
    in_specs = (
        P("rep", None, None),
        P("rep", None, None),
        P("rep", None),
        P(None, None, DP),
        P(DP, None),
    )
    out_specs = (P("rep", DP, None), P("rep", None, DP))

    def body(*args):
        return per_device(*args, dims)

    return jax.shard_map(
        body, mesh=split, in_specs=in_specs, out_specs=out_specs, check_vma=False
    )
```

```python
import jax
import jax.numpy as jnp
import numpy as np
from jax import lax
from jax.sharding import Mesh
from jax.sharding import PartitionSpec as P


DP = ("dp_0", "dp_1", "dp_2")
ALL = DP + ("rep",)
SWAP = [(0, 1), (1, 0)]
GRAD_SCALE = 0.03125
FIRST, SECOND = (1, 0), (0, 1)


def lines(dims, axis_of_core):
    index = np.arange(int(np.prod(dims))).reshape(dims)
    groups = []
    for core, axis in enumerate(axis_of_core):
        moved = np.moveaxis(index[..., core], axis, -1)
        groups += moved.reshape(-1, dims[axis]).tolist()
    return groups


def hop(value, dims, axis_of_core, step):
    pairs = []
    for line in lines(dims, axis_of_core):
        pairs += [(line[k], line[(k + step) % len(line)]) for k in range(len(line))]
    return lax.ppermute(value, ALL, sorted(pairs))


def exchange(value, dims, axis_of_core):
    groups = lines(dims, axis_of_core)
    return lax.all_to_all(value, ALL, 0, 0, tiled=True, axis_index_groups=groups)


def dot(a, b, over_a, over_b):
    return lax.dot_general(
        a, b, (((over_a,), (over_b,)), ((), ())), preferred_element_type=jnp.float32
    )


def per_device(tokens, cotangent, lengths, w_in, w_down, dims):
    ny, nx, nz, nr = dims
    x, dy = tokens[0], cotangent[0]
    rows, width = x.shape
    slots = rows // lengths.shape[1]
    units = w_down.shape[0]
    half = width // nr
    own_rows = rows // (ny * nx * nz)
    rep = lax.axis_index("rep")
    north = rep == 0
    me = jnp.where(north, lax.axis_index("dp_1"), lax.axis_index("dp_0"))
    across = jnp.where(north, lax.axis_index("dp_0"), lax.axis_index("dp_1"))
    one = jnp.minimum(lengths[0, 0], 1).astype(jnp.float32)

    w_t = w_in.transpose(1, 2, 0).reshape(2 * units, width)
    w_mine = lax.dynamic_slice_in_dim(w_t, rep * half, half, 1)
    w_gate, w_up = w_mine[:units].astype(jnp.float32), w_mine[units:].astype(jnp.float32)
    next_gate = hop(w_gate, dims, FIRST, -1)
    last_up = hop(w_up, dims, FIRST, 1)
    next_up = hop(w_up, dims, FIRST, -1)
    last_gate = hop(w_gate, dims, FIRST, 1)
    far_gate = hop(next_gate, dims, FIRST, -1)
    far_up = hop(last_up, dims, FIRST, 1)

    position = jnp.arange(rows)
    limit = jnp.where(position < slots, lengths[0, 0], slots + lengths[0, 1])
    is_alive = (position < limit)[None, :]
    gate_up = dot(w_t, x, 1, 1)
    gate, upward = gate_up[:units], gate_up[units:]
    sig = jax.nn.sigmoid(gate)
    activated = gate * sig
    hidden = jnp.where(is_alive, activated * upward, 0.0).astype(jnp.bfloat16)
    d_hidden = dot(w_down, dy, 1, 1)
    d_hidden = jnp.where(is_alive, d_hidden, 0.0)
    d_gate = d_hidden * upward * sig * (1.0 + gate * (1.0 - sig))
    d_up = d_hidden * activated
    d_in = jnp.concatenate([d_gate, d_up], axis=0).astype(jnp.bfloat16)

    each = rows // (ny * nx)
    order = (position // each % ny) * (nx * each) + (position // (ny * each)) * each + position % each
    turn = (position[:, None] == order[None, :]).astype(jnp.bfloat16)
    turned = dot(d_in, turn, 1, 0)
    plain = d_in.astype(jnp.float32)
    away, ours = jnp.where(north, plain, turned), jnp.where(north, turned, plain)
    theirs = lax.ppermute(away, "rep", SWAP)

    cols = rows // 4
    blocks = [jnp.concatenate([d[:, k * cols : (k + 1) * cols] for d in (ours, theirs)]) for k in range(4)]
    got = exchange(jnp.stack(blocks), dims, FIRST)
    picked = [lax.dynamic_index_in_dim(got, (me + k) & 3, 0, False) for k in range(4)]
    d_all = [(d * one).astype(jnp.bfloat16) for d in picked]

    g_in = dot(d_in, x, 1, 0)
    g_down = dot(hidden, dy, 1, 0)
    g = jnp.concatenate([g_in, g_down])
    low, high = g[:, :half], g[:, half:]
    away, kept = jnp.where(north, high, low), jnp.where(north, low, high)
    back = lax.ppermute(away, "rep", SWAP)

    arrived = lambda p: (p * one).astype(jnp.bfloat16)
    w_1 = jnp.concatenate([arrived(next_gate), arrived(next_up)])
    w_2 = jnp.concatenate([arrived(far_gate), arrived(far_up)])
    w_3 = jnp.concatenate([arrived(last_gate), arrived(last_up)])
    cut = half // 2

    def product(r):
        at = ((r + rep) & 1) * 2 * units
        d = [lax.dynamic_slice_in_dim(value, at, 2 * units, 0) for value in d_all]
        partial = dot(d[0], w_mine, 0, 0) + dot(d[1], w_1, 0, 0)
        partial = partial + dot(d[3], w_3, 0, 0) + dot(d[2], w_2, 0, 0)
        return partial.reshape(4, rows // 16, half)

    products = [product(r) for r in range(nr)]
    mine, b1, b2, b3 = (
        jnp.concatenate([lax.dynamic_index_in_dim(p, (across + k) & 3, 0, False) for p in products])
        for k in range(4)
    )
    r1 = hop(jnp.concatenate([b2[:, :cut], b1[:, cut:]], axis=1), dims, SECOND, 1)
    r2 = hop(jnp.concatenate([b3[:, :cut], b2[:, cut:]], axis=1), dims, SECOND, -1)
    up_2, down_2 = lax.optimization_barrier((b1[:, :cut] + r1[:, :cut], b3[:, cut:] + r2[:, cut:]))
    t1 = hop(up_2, dims, SECOND, 1)
    t2 = hop(down_2, dims, SECOND, -1)
    left = mine[:, :cut] + r2[:, :cut] + t1
    right = mine[:, cut:] + r1[:, cut:] + t2
    part = jnp.concatenate([left, right], axis=1).reshape(nr, nz, own_rows, half)
    iz = lax.axis_index("dp_2")
    at_z = lambda k: lax.dynamic_index_in_dim(part, (iz + k) & 7, 1, False).reshape(-1, half)
    b0, b1, b2, b3, b4, b5, b6, b7 = (at_z(k) for k in range(nz))
    along = (2, 2)
    ru = hop(jnp.concatenate([b3, b4[:, :cut]], axis=1), dims, along, 2)
    rd = hop(jnp.concatenate([b5, b4[:, cut:]], axis=1), dims, along, -2)
    near_up, near_down = b1 + ru[:, :half], b7 + rd[:, :half]
    far_up_sum = jnp.concatenate([b2[:, :cut] + ru[:, half:], b2[:, cut:]], axis=1)
    far_down_sum = jnp.concatenate([b6[:, :cut], b6[:, cut:] + rd[:, half:]], axis=1)
    near_up, near_down, far_up_sum, far_down_sum = lax.optimization_barrier(
        (near_up, near_down, far_up_sum, far_down_sum)
    )
    s2 = hop(far_up_sum, dims, along, 2)
    s6 = hop(far_down_sum, dims, along, -2)
    s1 = hop(near_up, dims, along, 1)
    s7 = hop(near_down, dims, along, -1)
    total = (b0 + s1 + s7 + s2 + s6).reshape(nr, own_rows, half)
    kept_half = lax.dynamic_index_in_dim(total, rep, 0, False)
    other_half = lax.ppermute(lax.dynamic_index_in_dim(total, 1 - rep, 0, False), "rep", SWAP)
    shard = jnp.concatenate(
        [jnp.where(north, kept_half, other_half), jnp.where(north, other_half, kept_half)], axis=1
    )
    shared = (kept + back) * GRAD_SCALE
    return shard[None], shared.reshape(3, units, half).transpose(2, 0, 1)


def solution(mesh):
    dims = (4, 4, 8, mesh.shape["rep"])
    split = Mesh(mesh.devices.reshape(dims), ALL)
    in_specs = (
        P("rep", None, None),
        P("rep", None, None),
        P("rep", None),
        P(None, None, DP),
        P(DP, None),
    )
    out_specs = (P("rep", DP, None), P("rep", None, DP))

    def body(*args):
        return per_device(*args, dims)

    return jax.shard_map(
        body, mesh=split, in_specs=in_specs, out_specs=out_specs, check_vma=False
    )
```

```python
import jax
import jax.numpy as jnp
import numpy as np
from jax import lax
from jax.sharding import Mesh
from jax.sharding import PartitionSpec as P


DP = ("dp_0", "dp_1", "dp_2")
ALL = DP + ("rep",)
SWAP = [(0, 1), (1, 0)]
GRAD_SCALE = 0.03125
FIRST, SECOND = (1, 0), (0, 1)


def lines(dims, axis_of_core):
    index = np.arange(int(np.prod(dims))).reshape(dims)
    groups = []
    for core, axis in enumerate(axis_of_core):
        moved = np.moveaxis(index[..., core], axis, -1)
        groups += moved.reshape(-1, dims[axis]).tolist()
    return groups


def hop(value, dims, axis_of_core, step):
    pairs = []
    for line in lines(dims, axis_of_core):
        pairs += [(line[k], line[(k + step) % len(line)]) for k in range(len(line))]
    return lax.ppermute(value, ALL, sorted(pairs))


def exchange(value, dims, axis_of_core):
    groups = lines(dims, axis_of_core)
    return lax.all_to_all(value, ALL, 0, 0, tiled=True, axis_index_groups=groups)


def dot(a, b, over_a, over_b):
    return lax.dot_general(
        a, b, (((over_a,), (over_b,)), ((), ())), preferred_element_type=jnp.float32
    )


def per_device(tokens, cotangent, lengths, w_in, w_down, dims):
    ny, nx, nz, nr = dims
    x, dy = tokens[0], cotangent[0]
    rows, width = x.shape
    slots = rows // lengths.shape[1]
    units = w_down.shape[0]
    half = width // nr
    own_rows = rows // (ny * nx * nz)
    rep = lax.axis_index("rep")
    north = rep == 0
    me = jnp.where(north, lax.axis_index("dp_1"), lax.axis_index("dp_0"))
    across = jnp.where(north, lax.axis_index("dp_0"), lax.axis_index("dp_1"))
    one = jnp.minimum(lengths[0, 0], 1).astype(jnp.float32)

    w_t = w_in.transpose(1, 2, 0).reshape(2 * units, width)
    w_mine = lax.dynamic_slice_in_dim(w_t, rep * half, half, 1)
    w_gate, w_up = w_mine[:units].astype(jnp.float32), w_mine[units:].astype(jnp.float32)
    next_gate = hop(w_gate, dims, FIRST, -1)
    last_up = hop(w_up, dims, FIRST, 1)
    next_up = hop(w_up, dims, FIRST, -1)
    last_gate = hop(w_gate, dims, FIRST, 1)
    far_gate = hop(next_gate, dims, FIRST, -1)
    far_up = hop(last_up, dims, FIRST, 1)

    position = jnp.arange(rows)
    limit = jnp.where(position < slots, lengths[0, 0], slots + lengths[0, 1])
    is_alive = (position < limit)[None, :]
    gate_up = dot(w_t, x, 1, 1)
    gate, upward = gate_up[:units], gate_up[units:]
    sig = jax.nn.sigmoid(gate)
    activated = gate * sig
    hidden = jnp.where(is_alive, activated * upward, 0.0).astype(jnp.bfloat16)
    d_hidden = dot(w_down, dy, 1, 1)
    d_hidden = jnp.where(is_alive, d_hidden, 0.0)
    d_gate = d_hidden * upward * sig * (1.0 + gate * (1.0 - sig))
    d_up = d_hidden * activated
    d_in = jnp.concatenate([d_gate, d_up], axis=0).astype(jnp.bfloat16)

    each = rows // (ny * nx)
    order = (position // each % ny) * (nx * each) + (position // (ny * each)) * each + position % each
    turn = (position[:, None] == order[None, :]).astype(jnp.bfloat16)
    turned = dot(d_in, turn, 1, 0)
    plain = d_in.astype(jnp.float32)
    away, ours = jnp.where(north, plain, turned), jnp.where(north, turned, plain)
    theirs = lax.ppermute(away, "rep", SWAP)

    cols = rows // 4
    blocks = [jnp.concatenate([d[:, k * cols : (k + 1) * cols] for d in (ours, theirs)]) for k in range(4)]
    got = exchange(jnp.stack(blocks), dims, FIRST)
    picked = [lax.dynamic_index_in_dim(got, (me + k) & 3, 0, False) for k in range(4)]
    d_all = [(d * one).astype(jnp.bfloat16) for d in picked]

    g_in = dot(d_in, x, 1, 0)
    g_down = dot(hidden, dy, 1, 0)
    g = jnp.concatenate([g_in, g_down])
    low, high = g[:, :half], g[:, half:]
    away, kept = jnp.where(north, high, low), jnp.where(north, low, high)
    back = lax.ppermute(away, "rep", SWAP)

    arrived = lambda p: (p * one).astype(jnp.bfloat16)
    w_1 = jnp.concatenate([arrived(next_gate), arrived(next_up)])
    w_2 = jnp.concatenate([arrived(far_gate), arrived(far_up)])
    w_3 = jnp.concatenate([arrived(last_gate), arrived(last_up)])
    cut = half // 2

    def product(r):
        at = ((r + rep) & 1) * 2 * units
        d = [lax.dynamic_slice_in_dim(value, at, 2 * units, 0) for value in d_all]
        partial = dot(d[0], w_mine, 0, 0) + dot(d[1], w_1, 0, 0)
        partial = partial + dot(d[3], w_3, 0, 0) + dot(d[2], w_2, 0, 0)
        return partial.reshape(4, rows // 16, half)

    parts = []
    for r in range(nr):
        p = product(r)
        mine, b1, b2, b3 = (lax.dynamic_index_in_dim(p, (across + k) & 3, 0, False) for k in range(4))
        r1 = hop(jnp.concatenate([b2[:, :cut], b1[:, cut:]], axis=1), dims, SECOND, 1)
        r2 = hop(jnp.concatenate([b3[:, :cut], b2[:, cut:]], axis=1), dims, SECOND, -1)
        up, down = b1[:, :cut] + r1[:, :cut], b3[:, cut:] + r2[:, cut:]
        up, down = lax.optimization_barrier((up, down))
        t1 = hop(up, dims, SECOND, 1)
        t2 = hop(down, dims, SECOND, -1)
        left = mine[:, :cut] + r2[:, :cut] + t1
        right = mine[:, cut:] + r1[:, cut:] + t2
        parts.append(jnp.concatenate([left, right], axis=1).reshape(nz, own_rows, half))
    iz = lax.axis_index("dp_2")
    at_z = lambda k: jnp.concatenate(
        [lax.dynamic_index_in_dim(part, (iz + k) & 7, 0, False) for part in parts]
    )
    b0, b1, b2, b3, b4, b5, b6, b7 = (at_z(k) for k in range(nz))
    along = (2, 2)
    ru = hop(jnp.concatenate([b3, b4[:, :cut]], axis=1), dims, along, 2)
    rd = hop(jnp.concatenate([b5, b4[:, cut:]], axis=1), dims, along, -2)
    near_up, near_down = b1 + ru[:, :half], b7 + rd[:, :half]
    far_up_sum = jnp.concatenate([b2[:, :cut] + ru[:, half:], b2[:, cut:]], axis=1)
    far_down_sum = jnp.concatenate([b6[:, :cut], b6[:, cut:] + rd[:, half:]], axis=1)
    near_up, far_up_sum = lax.optimization_barrier((near_up, far_up_sum))
    near_down, far_down_sum = lax.optimization_barrier((near_down, far_down_sum))
    s2 = hop(far_up_sum, dims, along, 2)
    s6 = hop(far_down_sum, dims, along, -2)
    s1 = hop(near_up, dims, along, 1)
    s7 = hop(near_down, dims, along, -1)
    total = (b0 + s1 + s7 + s2 + s6).reshape(nr, own_rows, half)
    kept_half = lax.dynamic_index_in_dim(total, rep, 0, False)
    other_half = lax.ppermute(lax.dynamic_index_in_dim(total, 1 - rep, 0, False), "rep", SWAP)
    shard = jnp.concatenate(
        [jnp.where(north, kept_half, other_half), jnp.where(north, other_half, kept_half)], axis=1
    )
    shared = (kept + back) * GRAD_SCALE
    return shard[None], shared.reshape(3, units, half).transpose(2, 0, 1)


def solution(mesh):
    dims = (4, 4, 8, mesh.shape["rep"])
    split = Mesh(mesh.devices.reshape(dims), ALL)
    in_specs = (
        P("rep", None, None),
        P("rep", None, None),
        P("rep", None),
        P(None, None, DP),
        P(DP, None),
    )
    out_specs = (P("rep", DP, None), P("rep", None, DP))

    def body(*args):
        return per_device(*args, dims)

    return jax.shard_map(
        body, mesh=split, in_specs=in_specs, out_specs=out_specs, check_vma=False
    )
```

```python
import jax
import jax.numpy as jnp
import numpy as np
from jax import lax
from jax.sharding import Mesh
from jax.sharding import PartitionSpec as P


DP = ("dp_0", "dp_1", "dp_2")
ALL = DP + ("rep",)
SWAP = [(0, 1), (1, 0)]
GRAD_SCALE = 0.03125
FIRST, SECOND = (1, 0), (0, 1)


def lines(dims, axis_of_core):
    index = np.arange(int(np.prod(dims))).reshape(dims)
    groups = []
    for core, axis in enumerate(axis_of_core):
        moved = np.moveaxis(index[..., core], axis, -1)
        groups += moved.reshape(-1, dims[axis]).tolist()
    return groups


def hop(value, dims, axis_of_core, step):
    pairs = []
    for line in lines(dims, axis_of_core):
        pairs += [(line[k], line[(k + step) % len(line)]) for k in range(len(line))]
    return lax.ppermute(value, ALL, sorted(pairs))


def exchange(value, dims, axis_of_core):
    groups = lines(dims, axis_of_core)
    return lax.all_to_all(value, ALL, 0, 0, tiled=True, axis_index_groups=groups)


def dot(a, b, over_a, over_b):
    return lax.dot_general(
        a, b, (((over_a,), (over_b,)), ((), ())), preferred_element_type=jnp.float32
    )


def per_device(tokens, cotangent, lengths, w_in, w_down, dims):
    ny, nx, nz, nr = dims
    x, dy = tokens[0], cotangent[0]
    rows, width = x.shape
    slots = rows // lengths.shape[1]
    units = w_down.shape[0]
    half = width // nr
    own_rows = rows // (ny * nx * nz)
    rep = lax.axis_index("rep")
    north = rep == 0
    me = jnp.where(north, lax.axis_index("dp_1"), lax.axis_index("dp_0"))
    across = jnp.where(north, lax.axis_index("dp_0"), lax.axis_index("dp_1"))
    one = jnp.minimum(lengths[0, 0], 1).astype(jnp.float32)

    w_t = w_in.transpose(1, 2, 0).reshape(2 * units, width)
    w_mine = lax.dynamic_slice_in_dim(w_t, rep * half, half, 1)
    w_gate, w_up = w_mine[:units].astype(jnp.float32), w_mine[units:].astype(jnp.float32)
    next_gate = hop(w_gate, dims, FIRST, -1)
    last_up = hop(w_up, dims, FIRST, 1)
    far_gate = hop(next_gate, dims, FIRST, -1)
    far_up = hop(last_up, dims, FIRST, 1)

    position = jnp.arange(rows)
    limit = jnp.where(position < slots, lengths[0, 0], slots + lengths[0, 1])
    is_alive = (position < limit)[None, :]
    gate_up = dot(w_t, x, 1, 1)
    gate_up, w_gate, w_up = lax.optimization_barrier((gate_up, w_gate, w_up))
    next_up = hop(w_up, dims, FIRST, -1)
    last_gate = hop(w_gate, dims, FIRST, 1)
    gate, upward = gate_up[:units], gate_up[units:]
    sig = jax.nn.sigmoid(gate)
    activated = gate * sig
    hidden = jnp.where(is_alive, activated * upward, 0.0).astype(jnp.bfloat16)
    d_hidden = dot(w_down, dy, 1, 1)
    d_hidden = jnp.where(is_alive, d_hidden, 0.0)
    d_gate = d_hidden * upward * sig * (1.0 + gate * (1.0 - sig))
    d_up = d_hidden * activated
    d_in = jnp.concatenate([d_gate, d_up], axis=0).astype(jnp.bfloat16)

    each = rows // (ny * nx)
    order = (position // each % ny) * (nx * each) + (position // (ny * each)) * each + position % each
    turn = (position[:, None] == order[None, :]).astype(jnp.bfloat16)
    turned = dot(d_in, turn, 1, 0)
    plain = d_in.astype(jnp.float32)
    away, ours = jnp.where(north, plain, turned), jnp.where(north, turned, plain)
    theirs = lax.ppermute(away, "rep", SWAP)

    cols = rows // 4
    blocks = [jnp.concatenate([d[:, k * cols : (k + 1) * cols] for d in (ours, theirs)]) for k in range(4)]
    got = exchange(jnp.stack(blocks), dims, FIRST)
    picked = [lax.dynamic_index_in_dim(got, (me + k) & 3, 0, False) for k in range(4)]
    d_all = [(d * one).astype(jnp.bfloat16) for d in picked]

    g_in = dot(d_in, x, 1, 0)
    g_down = dot(hidden, dy, 1, 0)
    g = jnp.concatenate([g_in, g_down])
    low, high = g[:, :half], g[:, half:]
    away, kept = jnp.where(north, high, low), jnp.where(north, low, high)
    back = lax.ppermute(away, "rep", SWAP)

    arrived = lambda p: (p * one).astype(jnp.bfloat16)
    w_1 = jnp.concatenate([arrived(next_gate), arrived(next_up)])
    w_2 = jnp.concatenate([arrived(far_gate), arrived(far_up)])
    w_3 = jnp.concatenate([arrived(last_gate), arrived(last_up)])
    cut = half // 2

    def product(r):
        at = ((r + rep) & 1) * 2 * units
        d = [lax.dynamic_slice_in_dim(value, at, 2 * units, 0) for value in d_all]
        partial = dot(d[0], w_mine, 0, 0) + dot(d[1], w_1, 0, 0)
        partial = partial + dot(d[3], w_3, 0, 0) + dot(d[2], w_2, 0, 0)
        return partial.reshape(4, rows // 16, half)

    parts = []
    for r in range(nr):
        p = product(r)
        mine, b1, b2, b3 = (lax.dynamic_index_in_dim(p, (across + k) & 3, 0, False) for k in range(4))
        r1 = hop(jnp.concatenate([b2[:, :cut], b1[:, cut:]], axis=1), dims, SECOND, 1)
        r2 = hop(jnp.concatenate([b3[:, :cut], b2[:, cut:]], axis=1), dims, SECOND, -1)
        up, down = b1[:, :cut] + r1[:, :cut], b3[:, cut:] + r2[:, cut:]
        up, down = lax.optimization_barrier((up, down))
        t1 = hop(up, dims, SECOND, 1)
        t2 = hop(down, dims, SECOND, -1)
        left = mine[:, :cut] + r2[:, :cut] + t1
        right = mine[:, cut:] + r1[:, cut:] + t2
        parts.append(jnp.concatenate([left, right], axis=1).reshape(nz, own_rows, half))
    iz = lax.axis_index("dp_2")
    at_z = lambda k: jnp.concatenate(
        [lax.dynamic_index_in_dim(part, (iz + k) & 7, 0, False) for part in parts]
    )
    b0, b1, b2, b3, b4, b5, b6, b7 = (at_z(k) for k in range(nz))
    along = (2, 2)
    ru = hop(jnp.concatenate([b3, b4[:, :cut]], axis=1), dims, along, 2)
    rd = hop(jnp.concatenate([b5, b4[:, cut:]], axis=1), dims, along, -2)
    near_up, near_down = b1 + ru[:, :half], b7 + rd[:, :half]
    far_up_sum = jnp.concatenate([b2[:, :cut] + ru[:, half:], b2[:, cut:]], axis=1)
    far_down_sum = jnp.concatenate([b6[:, :cut], b6[:, cut:] + rd[:, half:]], axis=1)
    near_up, near_down, far_up_sum, far_down_sum = lax.optimization_barrier(
        (near_up, near_down, far_up_sum, far_down_sum)
    )
    s2 = hop(far_up_sum, dims, along, 2)
    s6 = hop(far_down_sum, dims, along, -2)
    s1 = hop(near_up, dims, along, 1)
    s7 = hop(near_down, dims, along, -1)
    total = (b0 + s1 + s7 + s2 + s6).reshape(nr, own_rows, half)
    kept_half = lax.dynamic_index_in_dim(total, rep, 0, False)
    other_half = lax.ppermute(lax.dynamic_index_in_dim(total, 1 - rep, 0, False), "rep", SWAP)
    shard = jnp.concatenate(
        [jnp.where(north, kept_half, other_half), jnp.where(north, other_half, kept_half)], axis=1
    )
    shared = (kept + back) * GRAD_SCALE
    return shard[None], shared.reshape(3, units, half).transpose(2, 0, 1)


def solution(mesh):
    dims = (4, 4, 8, mesh.shape["rep"])
    split = Mesh(mesh.devices.reshape(dims), ALL)
    in_specs = (
        P("rep", None, None),
        P("rep", None, None),
        P("rep", None),
        P(None, None, DP),
        P(DP, None),
    )
    out_specs = (P("rep", DP, None), P("rep", None, DP))

    def body(*args):
        return per_device(*args, dims)

    return jax.shard_map(
        body, mesh=split, in_specs=in_specs, out_specs=out_specs, check_vma=False
    )
```
